256 devices in a mesh: dp: 4 (over y_hi, core), expert: 64 (over z, y_lo, x).
Axes of the slice: x: 4, y: 4 (y_hi: 2, y_lo: 2; y = y_hi * 2 + y_lo), z: 8, core: 2. Of those that a mesh axis runs over, the one named last changes fastest.
Arguments:
- student_latent: bfloat16 [32768, 1024], P(('dp', 'expert')), may hold values from -6 to 6
- target_latent: bfloat16 [32768, 1024], P(('dp', 'expert')), may hold values from -6 to 6
- student_gate: bfloat16 [64, 1024, 2048], P('expert', None, 'dp'), may hold values from -0.1875 to 0.1875
- student_up: bfloat16 [64, 1024, 2048], P('expert', None, 'dp'), may hold values from -0.1875 to 0.1875
- student_down: bfloat16 [64, 2048, 1024], P('expert', 'dp'), may hold values from -0.125 to 0.125
- target_gate: bfloat16 [64, 1024, 2048], P('expert', None, 'dp'), may hold values from -0.1875 to 0.1875
- target_up: bfloat16 [64, 1024, 2048], P('expert', None, 'dp'), may hold values from -0.1875 to 0.1875
- target_down: bfloat16 [64, 2048, 1024], P('expert', 'dp'), may hold values from -0.125 to 0.125
- student_routes: int32 [32768, 2], P(('dp', 'expert')), may hold values from 0 to 63, all different within a row; in each aligned block of 128 rows (0 to 127, 128 to 255, ...) at most 5 rows name the same one
- target_routes: int32 [32768, 2], P(('dp', 'expert')), may hold values from 0 to 63, all different within a row; in each aligned block of 128 rows (0 to 127, 128 to 255, ...) at most 5 rows name the same one
- student_mixing: float32 [32768, 2], P(('dp', 'expert')), may hold values from 0.1 to 1
- target_mixing: float32 [32768, 2], P(('dp', 'expert')), may hold values from 0.1 to 1
Outputs:
- gate_gradient: bfloat16 [64, 1024, 2048], P('expert', None, 'dp')
- up_gradient: bfloat16 [64, 1024, 2048], P('expert', None, 'dp')
- down_gradient: bfloat16 [64, 2048, 1024], P('expert', 'dp')
The draws below stay inside these ranges and needn't reach their ends.
Inputs may be any that keep to these rules, and one draw needn't show every extreme that they name: `student_routes`: each row names 2 different experts; within the 128 rows of one device (aligned blocks) no expert is named more than 5 times, a bound that some block reaches. `target_routes`: each row names 2 different experts; within the 128 rows of one device (aligned blocks) no expert is named more than 5 times, a bound that some block reaches.
All inputs are finite; a program needn't handle non-finite values.
Results may differ from the reference program's by a relative error of at most 0.012.
Values may be sent and summed in bfloat16 or wider, within the bound.
No kernel may reach another device: no remote copies, remote signals or barrier semaphores. Data moves between devices by JAX's collectives and lax.ppermute only.
A program may use at most 128 MiB of HBM per device.

```python
import math
import jax
import jax.numpy as jnp
import numpy as np
from jax import lax

D = 1024
FF = 2048
TOP = 2
TOK_DEV = 128
EXPERTS = 64
CAP = 5
TOKENS = 32768
N_DP = 4
N_EXPERT = 64


def level_of(stream_key, dims, pieces, smallest, largest):
    def one(dim, shards_of):
        steps = jax.random.uniform(jax.random.fold_in(jax.random.fold_in(stream_key, 6), dim), (shards_of,), jnp.float32, smallest / len(pieces), largest / len(pieces))
        return jnp.repeat(jnp.exp(steps), dims[dim] // shards_of).reshape((-1,) + (1,) * (len(dims) - dim - 1))

    factor_of = one(*pieces[0])
    for cut in pieces[1:]:
        factor_of = factor_of * one(*cut)
    return factor_of


def routed_block(key, own, number, rows, count, top, reach, skew):
    ranking = jax.random.permutation(key, count)
    crowded, ordinary = portions_of(count, rows * top, reach, skew, True), portions_of(count, rows * top, reach, skew, False)
    places = jnp.arange(count)

    def named(lengths, turn):
        used = int((lengths > 0).sum())
        fixed = max(1, used // 4)
        shifted = fixed + (places - fixed + turn * (used - fixed)) % max(1, count - fixed)
        return jnp.zeros((count,), jnp.int32).at[ranking[jnp.where(places < fixed, places, shifted)]].set(jnp.asarray(lengths, jnp.int32))

    lengths = jnp.where(number % 4 == 0, named(crowded, number // 4), named(ordinary, number - number // 4 - 1))
    mixed = jax.random.permutation(jax.random.fold_in(own, 3), count)
    source_of, sink = mixed[0:count // 2 * 2:2], mixed[1:count // 2 * 2:2]
    margin = jnp.minimum(lengths[source_of] - 1, reach - lengths[sink]) // 2
    margin = jnp.where((source_of == ranking[0]) | (sink == ranking[0]) | (lengths[sink] == 0), 0, jnp.maximum(margin, 0))
    shifted = jax.random.randint(jax.random.fold_in(own, 4), (count // 2,), 0, 1 << 20) % (margin + 1)
    lengths = lengths.at[source_of].add(-shifted).at[sink].add(shifted)
    items = jnp.searchsorted(jnp.cumsum(lengths), jnp.arange(rows * top), side="right").astype(jnp.int32)
    table = items.reshape(top, rows).T
    table = table[jax.random.permutation(jax.random.fold_in(own, 1), rows)]
    turn = jax.random.randint(jax.random.fold_in(own, 2), (rows, 1), 0, top)
    return jnp.take_along_axis(table, (jnp.arange(top)[None, :] + turn) % top, axis=1)


def portions_of(count, total, most, slope, full):
    portions = [(1 << 20) // math.isqrt(grade ** slope) + 1 for grade in range(1, count + 1)]
    largest = most if full else min(most, max(-(-total // count), total * portions[0] // sum(portions)))
    least = 1 if total - largest >= count - 1 else 0
    given, surplus = [largest] + [least] * (count - 1), total - largest - least * (count - 1)
    while surplus > 0:
        candidates = [i for i in range(1, count) if given[i] < largest] or [i for i in range(1, count) if given[i] < most]
        mass, budget = sum([portions[i] for i in candidates]), surplus
        for i in candidates:
            extra = min(most - given[i], max(1, budget * portions[i] // mass), surplus)
            given[i] = given[i] + extra
            surplus = surplus - extra
    return np.array(given)


def normal_values(stream_key, extent, deviation, limit, split=(), kind=jnp.bfloat16):
    entries = jax.random.normal(stream_key, extent, jnp.float32) * deviation
    if len(split) > 0:
        entries = level_of(stream_key, extent, split, -0.22, 0.18) * entries
    return jnp.clip(entries, min=-limit, max=limit).astype(kind)


def setup_inputs(seed: int = 0) -> dict:
    arg_keys = jax.random.split(jax.random.key(seed), 13)
    student_latent = normal_values(arg_keys[0], (TOKENS, D), 1.0, 6.0, ((0, 256),))
    target_latent = normal_values(arg_keys[1], (TOKENS, D), 1.0, 6.0, ((0, 256),))
    student_gate = normal_values(arg_keys[2], (EXPERTS, D, FF), D ** -0.5, 0.1875, ((0, 64), (2, 4)))
    student_up = normal_values(arg_keys[3], (EXPERTS, D, FF), D ** -0.5, 0.1875, ((0, 64), (2, 4)))
    student_down = normal_values(arg_keys[4], (EXPERTS, FF, D), FF ** -0.5, 0.125, ((0, 64), (1, 4)))
    target_gate = normal_values(arg_keys[5], (EXPERTS, D, FF), D ** -0.5, 0.1875, ((0, 64), (2, 4)))
    target_up = normal_values(arg_keys[6], (EXPERTS, D, FF), D ** -0.5, 0.1875, ((0, 64), (2, 4)))
    target_down = normal_values(arg_keys[7], (EXPERTS, FF, D), FF ** -0.5, 0.125, ((0, 64), (1, 4)))
    student_routes_keys = jax.random.split(jax.random.fold_in(arg_keys[8], 1), TOKENS // TOK_DEV)
    student_routes_turns = jax.random.permutation(jax.random.fold_in(arg_keys[8], 3), TOKENS // TOK_DEV)
    student_routes = jax.vmap(lambda own, number: routed_block(jax.random.fold_in(arg_keys[8], 2), own, number, TOK_DEV, EXPERTS, TOP, CAP, 2))(student_routes_keys, student_routes_turns).reshape((TOKENS, TOP))
    target_routes_keys = jax.random.split(jax.random.fold_in(arg_keys[9], 1), TOKENS // TOK_DEV)
    target_routes_turns = jax.random.permutation(jax.random.fold_in(arg_keys[9], 3), TOKENS // TOK_DEV)
    target_routes = jax.vmap(lambda own, number: routed_block(jax.random.fold_in(arg_keys[9], 2), own, number, TOK_DEV, EXPERTS, TOP, CAP, 2))(target_routes_keys, target_routes_turns).reshape((TOKENS, TOP))
    student_mixing = jnp.clip(jnp.exp(math.log(1.0) - 2.3025851 * jax.random.uniform(arg_keys[10], (TOKENS, TOP), jnp.float32) ** level_of(arg_keys[10], (TOKENS, TOP), ((0, 256),), -0.2, 0.2)), 0.1, 1.0)
    target_mixing = jnp.clip(jnp.exp(math.log(1.0) - 2.3025851 * jax.random.uniform(arg_keys[11], (TOKENS, TOP), jnp.float32) ** level_of(arg_keys[11], (TOKENS, TOP), ((0, 256),), -0.2, 0.2)), 0.1, 1.0)
    return dict(student_latent=student_latent, target_latent=target_latent, student_gate=student_gate, student_up=student_up, student_down=student_down, target_gate=target_gate, target_up=target_up, target_down=target_down, student_routes=student_routes, target_routes=target_routes, student_mixing=student_mixing, target_mixing=target_mixing)


def rms_rows(latent):
    widened = latent.astype(jnp.float32)
    factor = lax.rsqrt(lax.optimization_barrier(jnp.mean(widened * widened, axis=1, keepdims=True)) + 1e-06)
    return (widened * factor).astype(jnp.bfloat16)

def slot_tables(routes):
    devices = N_DP * N_EXPERT
    labels = routes.reshape(devices, TOK_DEV * TOP)
    experts_list = jnp.arange(EXPERTS, dtype=jnp.int32)
    onehot = (labels[:, :, None] == experts_list[None, None, :]).astype(jnp.int32)
    before = jnp.cumsum(onehot, axis=1) - onehot
    position = lax.optimization_barrier(jnp.sum(before * onehot, axis=2))
    owners = jnp.arange(devices, dtype=jnp.int32)[:, None]
    placed = ((labels * devices + owners) * CAP + position).reshape(-1)
    total_rows = TOKENS * TOP
    source = jnp.full((EXPERTS * devices * CAP,), total_rows, jnp.int32)
    source = source.at[placed].set(jnp.arange(total_rows, dtype=jnp.int32))
    return (placed, source.reshape(EXPERTS, devices * CAP))

def pad_rows(values):
    return jnp.concatenate([values, jnp.zeros((1, values.shape[1]), values.dtype)], axis=0)

def forward_parts(gathered, gate_w, up_w):
    pre_gate = jnp.dot(gathered, gate_w, preferred_element_type=jnp.float32)
    pre_up = jnp.dot(gathered, up_w, preferred_element_type=jnp.float32)
    hidden = (jax.nn.silu(pre_gate) * pre_up).astype(jnp.bfloat16)
    return (pre_gate, pre_up, hidden)

def quarter_sums(hidden, down_w):
    rows = hidden.shape[0]
    parts_hidden = hidden.reshape(rows, N_DP, FF // N_DP).astype(jnp.float32)
    parts_down = down_w.reshape(N_DP, FF // N_DP, D).astype(jnp.float32)
    partial_value = jnp.einsum('rgf,gfd->grd', parts_hidden, parts_down).astype(jnp.bfloat16)
    return lax.optimization_barrier(jnp.sum(partial_value.astype(jnp.float32), axis=0)).astype(jnp.bfloat16)

def expert_outputs(normed, source, gate_all, up_all, down_all):
    padded = pad_rows(normed)

    def one_expert(operands):
        sources, gate_w, up_w, down_w = operands
        gathered = jnp.take(padded, sources // TOP, axis=0)
        hidden = forward_parts(gathered, gate_w, up_w)[2]
        return quarter_sums(hidden, down_w)
    return lax.map(one_expert, (source, gate_all, up_all, down_all))

def layer_output(latent, mixing, placed, outputs):
    picked = jnp.take(outputs.reshape(-1, D), placed, axis=0).reshape(TOKENS, TOP, D)
    return latent.astype(jnp.float32) + lax.optimization_barrier(jnp.sum(mixing[:, :, None] * picked.astype(jnp.float32), axis=1))

def expert_grads(normed, slot_values, source, gate_all, up_all, down_all):
    padded = pad_rows(normed)
    padded_slots = pad_rows(slot_values)

    def one_expert(operands):
        sources, gate_w, up_w, down_w = operands
        gathered = jnp.take(padded, sources // TOP, axis=0)
        returned = jnp.take(padded_slots, sources, axis=0)
        pre_gate, pre_up, hidden = forward_parts(gathered, gate_w, up_w)
        down_part = lax.dot_general(hidden, returned, (((0,), (0,)), ((), ())), preferred_element_type=jnp.float32)
        grad_hidden = lax.dot_general(returned, down_w, (((1,), (1,)), ((), ())), preferred_element_type=jnp.float32)
        sigmoid_gate = jax.nn.sigmoid(pre_gate)
        grad_pre_gate = (grad_hidden * pre_up * sigmoid_gate * (1.0 + pre_gate * (1.0 - sigmoid_gate))).astype(jnp.bfloat16)
        grad_pre_up = (grad_hidden * pre_gate * sigmoid_gate).astype(jnp.bfloat16)
        gate_part = lax.dot_general(gathered, grad_pre_gate, (((0,), (0,)), ((), ())), preferred_element_type=jnp.float32)
        up_part = lax.dot_general(gathered, grad_pre_up, (((0,), (0,)), ((), ())), preferred_element_type=jnp.float32)
        return (gate_part.astype(jnp.bfloat16), up_part.astype(jnp.bfloat16), down_part.astype(jnp.bfloat16))
    return lax.map(one_expert, (source, gate_all, up_all, down_all))

def reference(student_latent, target_latent, student_gate, student_up, student_down, target_gate, target_up, target_down, student_routes, target_routes, student_mixing, target_mixing):
    normed_student = rms_rows(student_latent)
    normed_target = rms_rows(target_latent)
    placed_student, source_student = slot_tables(student_routes)
    placed_target, source_target = slot_tables(target_routes)
    student_expert = expert_outputs(normed_student, source_student, student_gate, student_up, student_down)
    target_expert = expert_outputs(normed_target, source_target, target_gate, target_up, target_down)
    student_out = layer_output(student_latent, student_mixing, placed_student, student_expert)
    target_out = layer_output(target_latent, target_mixing, placed_target, target_expert)
    factor = (EXPERTS / (TOP * TOKENS)) ** 0.5
    cotangent = factor * (student_out - target_out)
    slot_cotangent = (student_mixing[:, :, None] * cotangent[:, None, :]).astype(jnp.bfloat16).reshape(TOKENS * TOP, D)
    gate_gradient, up_gradient, down_gradient = expert_grads(normed_student, slot_cotangent, source_student, student_gate, student_up, student_down)
    return (gate_gradient, up_gradient, down_gradient)
```

```python
import functools
import jax
import jax.numpy as jnp
from jax import lax
from jax.experimental import pallas as pl
from jax.experimental.pallas import tpu as pltpu
from jax.sharding import PartitionSpec as P


F32 = jnp.float32
BF16 = jnp.bfloat16
LANES = 128


def params(mib):
    return pltpu.CompilerParams(vmem_limit_bytes=mib * 1024 * 1024)


def call(body, outs, scratch=(), mib=32, cost=None, **more):
    return pl.pallas_call(
        body,
        out_shape=outs,
        scratch_shapes=list(scratch),
        compiler_params=params(mib),
        cost_estimate=pl.CostEstimate(flops=cost or 1, bytes_accessed=1 << 20, transcendentals=0),
        **more,
    )


def store_flat(value, scratch):
    rows, width = value.shape
    pieces = width // LANES
    for c in range(pieces):
        scratch[pl.ds(c, rows, stride=pieces), :] = value[:, c * LANES : (c + 1) * LANES]


def load_flat(scratch, pieces, c):
    return scratch[pl.ds(c, scratch.shape[0] // pieces, stride=pieces), :]


def column(rows, k):
    n = rows.shape[1]
    return jnp.broadcast_to(rows[k : k + 1, :], (n, n)).T[:, :1]


def places(routes, experts, capacity):
    tokens = routes.shape[1]
    lane = lax.broadcasted_iota(jnp.int32, (tokens, experts), 1)
    chosen = [column(routes.astype(F32), k).astype(jnp.int32) for k in range(2)]
    hot = [(c == lane).astype(F32) for c in chosen]
    earlier = (
        lax.broadcasted_iota(jnp.int32, (tokens, tokens), 1)
        < lax.broadcasted_iota(jnp.int32, (tokens, tokens), 0)
    ).astype(BF16)
    before = [jnp.dot(earlier, h.astype(BF16), preferred_element_type=F32) for h in hot]
    before[1] = before[1] + jnp.sum(hot[0], axis=0, keepdims=True)
    slot = lax.broadcasted_iota(jnp.int32, (tokens, experts * capacity), 1)
    found = []
    for k in range(2):
        position = jnp.sum(before[k] * hot[k], axis=1, keepdims=True).astype(jnp.int32)
        found.append((slot == chosen[k] * capacity + position).astype(BF16))
    return found


def turned_dot(a, b):
    return lax.dot_general(a, b, (((0,), (0,)), ((), ())), preferred_element_type=F32)


def pack_body(experts, capacity, *refs):
    packed, scratch = refs[-2:]
    sets = len(refs) // 2 - 1
    deep = packed.shape[1] // sets
    for i in range(sets):
        latent, routes = refs[2 * i : 2 * i + 2]
        wide = latent[...].astype(F32)
        scale = lax.rsqrt(jnp.mean(wide * wide, axis=1, keepdims=True) + 1e-06)
        normed = (wide * scale).astype(BF16)
        first, second = places(routes[...], experts, capacity)
        store_flat(turned_dot(first + second, normed), scratch)
        packed[:, i * deep : (i + 1) * deep, :] = (
            scratch[...].reshape(experts, deep, LANES).astype(BF16)
        )


def forward_body(flat, gate, up, down, gate2, up2, down2, rows, partial, scratch, total):
    j = pl.program_id(0)
    pieces = rows.shape[1] // LANES

    @pl.when(j == 0)
    def _():
        scratch[...] = flat[...].astype(F32).reshape(scratch.shape)
        for c in range(pieces):
            rows[:, c * LANES : (c + 1) * LANES] = load_flat(scratch, pieces, c).astype(BF16)

    x = rows[...]
    found = None
    for g, u, d in ((gate, up, down), (gate2, up2, down2)):
        pre_gate = jnp.dot(x, g[0], preferred_element_type=F32)
        pre_up = jnp.dot(x, u[0], preferred_element_type=F32)
        hidden = (jax.nn.silu(pre_gate) * pre_up).astype(BF16)
        part = jnp.dot(hidden, d[0], preferred_element_type=F32)
        found = part if found is None else found + part

    @pl.when(j == 0)
    def _():
        total[...] = found

    @pl.when(j == pl.num_programs(0) - 1)
    def _():
        store_flat(total[...] + found, scratch)
        partial[...] = scratch[...].reshape(partial.shape).astype(partial.dtype)


def forward(flat, part, parts, mine, other, width, dtype):
    steps = 2
    experts, deep = flat.shape[0], flat.shape[1] // parts
    count = experts * deep * LANES // width
    hidden = mine[0].shape[2]
    cut = hidden // steps
    across = pl.BlockSpec((1, width, cut), lambda j: (0, 0, j))
    down = pl.BlockSpec((1, cut, width), lambda j: (0, j, 0))
    return call(
        forward_body,
        (
            jax.ShapeDtypeStruct((count, width), BF16),
            jax.ShapeDtypeStruct((experts, deep, LANES), dtype),
        ),
        (pltpu.VMEM((experts * deep, LANES), F32), pltpu.VMEM((count, width), F32)),
        mib=62,
        cost=12 * count * width * hidden,
        grid=(steps,),
        in_specs=[
            pl.BlockSpec((experts, deep, LANES), lambda j: (0, part, 0)),
            across, across, down, across, across, down,
        ],
        out_specs=(
            pl.BlockSpec((count, width), lambda j: (0, 0)),
            pl.BlockSpec((experts, deep, LANES), lambda j: (0, 0, 0)),
        ),
    )(flat, *mine, *other)


def factors_body(rows, gate, up, turned_rows, turned_hidden, by_gate, by_up):
    x = rows[...]
    pre_gate = jnp.dot(x, gate[0], preferred_element_type=F32)
    pre_up = jnp.dot(x, up[0], preferred_element_type=F32)
    s = jax.nn.sigmoid(pre_gate)
    through = pre_gate * s
    by_gate[...] = pre_up * s * (1.0 + pre_gate * (1.0 - s))
    by_up[...] = through
    turned_hidden[...] = (through * pre_up).astype(BF16).T
    turned_rows[...] = x.T


def factors(rows, gate, up):
    count, width = rows.shape
    hidden = gate.shape[2]
    cut = 256
    held = pl.BlockSpec((1, width, hidden), lambda i: (0, 0, 0))
    return call(
        factors_body,
        (
            jax.ShapeDtypeStruct((width, count), BF16),
            jax.ShapeDtypeStruct((hidden, count), BF16),
            jax.ShapeDtypeStruct((count, hidden), F32),
            jax.ShapeDtypeStruct((count, hidden), F32),
        ),
        mib=62,
        cost=4 * count * width * hidden,
        grid=(count // cut,),
        in_specs=[pl.BlockSpec((cut, width), lambda i: (i, 0)), held, held],
        out_specs=(
            pl.BlockSpec((width, cut), lambda i: (0, i)),
            pl.BlockSpec((hidden, cut), lambda i: (0, i)),
            pl.BlockSpec((cut, hidden), lambda i: (i, 0)),
            pl.BlockSpec((cut, hidden), lambda i: (i, 0)),
        ),
    )(rows, gate, up)


def combine_body(
    experts, capacity, factor, s_flat, t_flat, s_latent, t_latent, s_routes, t_routes, s_mixing,
    t_mixing, packed, scratch, gathered,
):
    pieces = s_latent.shape[1] // LANES
    found = []
    for flat, latent, routes, mixing in (
        (s_flat, s_latent, s_routes, s_mixing),
        (t_flat, t_latent, t_routes, t_mixing),
    ):
        scratch[...] = flat[...].astype(F32).reshape(scratch.shape)
        for c in range(pieces):
            gathered[:, c * LANES : (c + 1) * LANES] = load_flat(scratch, pieces, c).astype(BF16)
        where = places(routes[...], experts, capacity)
        mixed = [column(mixing[...], k) for k in range(2)]
        picked = [
            jnp.dot(w, gathered[...], preferred_element_type=F32) * mixed[k]
            for k, w in enumerate(where)
        ]
        found.append((latent[...].astype(F32) + (picked[0] + picked[1]), where, mixed))
    cotangent = factor * (found[0][0] - found[1][0])
    where, mixed = found[0][1:]
    slots = [
        turned_dot(w, (mixed[k] * cotangent).astype(BF16)) for k, w in enumerate(where)
    ]
    store_flat(slots[0] + slots[1], scratch)
    packed[...] = scratch[...].reshape(packed.shape).astype(BF16)


def backward_body(last, *refs):
    one, two, down, turned_rows, turned_hidden, by_gate, by_up = refs[:7]
    earlier = refs[7:10] if last else (None,) * 3
    gate_out, up_out, down_out, scratch, cotangent = refs[-5:]
    pieces = down.shape[2] // LANES

    @pl.when(pl.program_id(0) == 0)
    def _():
        count = cotangent.shape[0] // 2
        for b, flat in enumerate((one, two)):
            scratch[...] = flat[...].astype(F32).reshape(scratch.shape)
            for c in range(pieces):
                cotangent[b * count : (b + 1) * count, c * LANES : (c + 1) * LANES] = load_flat(
                    scratch, pieces, c
                ).astype(BF16)

    back = cotangent[...]
    grad_hidden = lax.dot_general(
        back, down[0], (((1,), (1,)), ((), ())), preferred_element_type=F32
    )
    grad_gate = (grad_hidden * by_gate[...]).astype(BF16)
    grad_up = (grad_hidden * by_up[...]).astype(BF16)
    for out, before, left, right in (
        (gate_out, earlier[0], turned_rows, grad_gate),
        (up_out, earlier[1], turned_rows, grad_up),
        (down_out, earlier[2], turned_hidden, back),
    ):
        found = jnp.dot(left[...], right, preferred_element_type=F32)
        out[0] = (found if before is None else found + before[0]).astype(out.dtype)


def backward(blocks, turn, down, turned_rows, turned_hidden, by_gate, by_up, earlier=()):
    steps = 2
    hidden, width = down.shape[1:]
    count = turned_rows.shape[1] // 2
    cut = hidden // steps
    dtype = BF16 if earlier else F32
    flat = pl.BlockSpec(blocks[0].shape, lambda j: (0, 0, 0))
    flat_rows = blocks[0].shape[0] * blocks[0].shape[1]
    grads = [
        pl.BlockSpec((1, width, cut), lambda j: (0, 0, j)),
        pl.BlockSpec((1, width, cut), lambda j: (0, 0, j)),
        pl.BlockSpec((1, cut, width), lambda j: (0, j, 0)),
    ]
    return call(
        functools.partial(backward_body, bool(earlier)),
        (
            jax.ShapeDtypeStruct((1, width, hidden), dtype),
            jax.ShapeDtypeStruct((1, width, hidden), dtype),
            jax.ShapeDtypeStruct((1, hidden, width), dtype),
        ),
        (pltpu.VMEM((flat_rows, LANES), F32), pltpu.VMEM((count, width), BF16)),
        cost=4 * count * 2 * width * hidden,
        grid=(steps,),
        in_specs=[
            flat, flat,
            pl.BlockSpec((1, cut, width), lambda j: (0, j, 0)),
            pl.BlockSpec((width, count), lambda j: (0, turn)),
            pl.BlockSpec((cut, count), lambda j: (j, turn)),
            pl.BlockSpec((count, cut), lambda j: (turn, j)),
            pl.BlockSpec((count, cut), lambda j: (turn, j)),
            *(grads if earlier else ()),
        ],
        out_specs=tuple(grads),
    )(*blocks, down, turned_rows, turned_hidden, by_gate, by_up, *earlier)


def to_experts(blocks):
    return lax.all_to_all(blocks, "expert", split_axis=0, concat_axis=0, tiled=True)


def other_core(value):
    return lax.ppermute(value, "dp", ((0, 1), (1, 0), (2, 3), (3, 2)))


def other_chip(value):
    return lax.ppermute(value, "dp", ((0, 2), (2, 0), (1, 3), (3, 1)))


def shards(
    student_latent,
    target_latent,
    student_gate,
    student_up,
    student_down,
    target_gate,
    target_up,
    target_down,
    student_routes,
    target_routes,
    student_mixing,
    target_mixing,
):
    groups = lax.axis_size("dp")
    experts = lax.axis_size("expert")
    tokens, width = student_latent.shape
    top = student_routes.shape[1]
    capacity = tokens * top * 5 // (4 * experts)
    slots = experts * capacity
    deep = capacity * width // LANES
    flat_shape = (experts * deep, LANES)
    blocks_shape = (experts, deep, LANES)

    def packing(*sets):
        return call(
            functools.partial(pack_body, experts, capacity),
            jax.ShapeDtypeStruct((experts, len(sets) // 2 * deep, LANES), BF16),
            (pltpu.VMEM(flat_shape, F32),),
            mib=12,
            cost=2 * tokens * slots * width,
        )(*sets)

    student_routes, target_routes = student_routes.T, target_routes.T
    student_mixing, target_mixing = student_mixing.T, target_mixing.T
    far_latent = other_chip(target_latent)
    far_routes = other_chip(target_routes)
    sent_student = packing(student_latent, student_routes)
    sent_target = packing(target_latent, target_routes, far_latent, far_routes)
    own_student = to_experts(sent_student)
    both_target = to_experts(sent_target)
    student = (student_gate, student_up, student_down)
    target = (target_gate, target_up, target_down)
    student2 = tuple(other_core(w) for w in student)
    target2 = tuple(other_core(w) for w in target)
    far_student = other_chip(own_student)

    own_rows, own_part = forward(own_student, 0, 1, student, student2, width, F32)
    far_rows, far_part = forward(far_student, 0, 1, student, student2, width, BF16)
    own_part_t = forward(both_target, 0, 2, target, target2, width, F32)[1]
    far_part_t = forward(both_target, 1, 2, target, target2, width, BF16)[1]
    came_s = other_chip(far_part)
    came_t = other_chip(far_part_t)
    student_sum = (own_part + came_s.astype(F32)).astype(BF16)
    target_sum = (own_part_t + came_t.astype(F32)).astype(BF16)
    back_student = to_experts(student_sum)
    back_target = to_experts(target_sum)

    rows = jnp.concatenate([own_rows, other_core(own_rows), far_rows, other_core(far_rows)], axis=0)
    turned_rows, turned_hidden, by_gate, by_up = factors(rows, student_gate, student_up)

    factor = (experts / (top * tokens * groups * experts)) ** 0.5
    slot_values = call(
        functools.partial(combine_body, experts, capacity, factor),
        jax.ShapeDtypeStruct(blocks_shape, BF16),
        (pltpu.VMEM(flat_shape, F32), pltpu.VMEM((slots, width), BF16)),
        mib=16,
        cost=8 * tokens * slots * width,
    )(
        back_student, back_target, student_latent, target_latent, student_routes,
        target_routes, student_mixing, target_mixing,
    )
    own_cot = to_experts(slot_values)
    far_cot = other_chip(own_cot)
    own_cot2 = other_core(own_cot)
    given = (student_down, turned_rows, turned_hidden, by_gate, by_up)
    near = backward((own_cot, own_cot2), 0, *given)
    far_cot2 = other_core(far_cot)
    return backward((far_cot, far_cot2), 1, *given, tuple(near))


def solution(mesh):
    in_specs = (
        P(("dp", "expert"), None),
        P(("dp", "expert"), None),
        P("expert", None, "dp"),
        P("expert", None, "dp"),
        P("expert", "dp", None),
        P("expert", None, "dp"),
        P("expert", None, "dp"),
        P("expert", "dp", None),
        P(("dp", "expert"), None),
        P(("dp", "expert"), None),
        P(("dp", "expert"), None),
        P(("dp", "expert"), None),
    )
    out_specs = (P("expert", None, "dp"), P("expert", None, "dp"), P("expert", "dp", None))
    return jax.shard_map(shards, mesh=mesh, in_specs=in_specs, out_specs=out_specs, check_vma=False)
```

```python
import functools
import jax
import jax.numpy as jnp
from jax import lax
from jax.experimental import pallas as pl
from jax.experimental.pallas import tpu as pltpu
from jax.sharding import PartitionSpec as P


F32 = jnp.float32
BF16 = jnp.bfloat16
LANES = 128


def params(mib):
    return pltpu.CompilerParams(vmem_limit_bytes=mib * 1024 * 1024)


def call(body, outs, scratch=(), mib=32, cost=None, **more):
    return pl.pallas_call(
        body,
        out_shape=outs,
        scratch_shapes=list(scratch),
        compiler_params=params(mib),
        cost_estimate=pl.CostEstimate(flops=cost or 1, bytes_accessed=1 << 20, transcendentals=0),
        **more,
    )


def store_flat(value, scratch):
    rows, width = value.shape
    pieces = width // LANES
    for c in range(pieces):
        scratch[pl.ds(c, rows, stride=pieces), :] = value[:, c * LANES : (c + 1) * LANES]


def load_flat(scratch, pieces, c):
    return scratch[pl.ds(c, scratch.shape[0] // pieces, stride=pieces), :]


def column(rows, k):
    n = rows.shape[1]
    return jnp.broadcast_to(rows[k : k + 1, :], (n, n)).T[:, :1]


def places(routes, experts, capacity):
    tokens = routes.shape[1]
    lane = lax.broadcasted_iota(jnp.int32, (tokens, experts), 1)
    chosen = [column(routes.astype(F32), k).astype(jnp.int32) for k in range(2)]
    hot = [(c == lane).astype(F32) for c in chosen]
    earlier = (
        lax.broadcasted_iota(jnp.int32, (tokens, tokens), 1)
        < lax.broadcasted_iota(jnp.int32, (tokens, tokens), 0)
    ).astype(BF16)
    before = [jnp.dot(earlier, h.astype(BF16), preferred_element_type=F32) for h in hot]
    before[1] = before[1] + jnp.sum(hot[0], axis=0, keepdims=True)
    slot = lax.broadcasted_iota(jnp.int32, (tokens, experts * capacity), 1)
    found = []
    for k in range(2):
        position = jnp.sum(before[k] * hot[k], axis=1, keepdims=True).astype(jnp.int32)
        found.append((slot == chosen[k] * capacity + position).astype(BF16))
    return found


def turned_dot(a, b):
    return lax.dot_general(a, b, (((0,), (0,)), ((), ())), preferred_element_type=F32)


def pack_body(experts, capacity, *refs):
    packed, scratch = refs[-2:]
    sets = len(refs) // 2 - 1
    deep = packed.shape[1] // sets
    for i in range(sets):
        latent, routes = refs[2 * i : 2 * i + 2]
        wide = latent[...].astype(F32)
        scale = lax.rsqrt(jnp.mean(wide * wide, axis=1, keepdims=True) + 1e-06)
        normed = (wide * scale).astype(BF16)
        first, second = places(routes[...], experts, capacity)
        store_flat(turned_dot(first + second, normed), scratch)
        packed[:, i * deep : (i + 1) * deep, :] = (
            scratch[...].reshape(experts, deep, LANES).astype(BF16)
        )


def forward_body(flat, gate, up, down, gate2, up2, down2, rows, partial, scratch, total):
    j = pl.program_id(0)
    pieces = rows.shape[1] // LANES

    @pl.when(j == 0)
    def _():
        scratch[...] = flat[...].astype(F32).reshape(scratch.shape)
        for c in range(pieces):
            rows[:, c * LANES : (c + 1) * LANES] = load_flat(scratch, pieces, c).astype(BF16)

    x = rows[...]
    found = None
    for g, u, d in ((gate, up, down), (gate2, up2, down2)):
        pre_gate = jnp.dot(x, g[0], preferred_element_type=F32)
        pre_up = jnp.dot(x, u[0], preferred_element_type=F32)
        hidden = (jax.nn.silu(pre_gate) * pre_up).astype(BF16)
        part = jnp.dot(hidden, d[0], preferred_element_type=F32)
        found = part if found is None else found + part

    @pl.when(j == 0)
    def _():
        total[...] = found

    @pl.when(j == pl.num_programs(0) - 1)
    def _():
        store_flat(total[...] + found, scratch)
        partial[...] = scratch[...].reshape(partial.shape).astype(partial.dtype)


def forward(flat, part, parts, mine, other, width, dtype):
    steps = 2
    experts, deep = flat.shape[0], flat.shape[1] // parts
    count = experts * deep * LANES // width
    hidden = mine[0].shape[2]
    cut = hidden // steps
    across = pl.BlockSpec((1, width, cut), lambda j: (0, 0, j))
    down = pl.BlockSpec((1, cut, width), lambda j: (0, j, 0))
    return call(
        forward_body,
        (
            jax.ShapeDtypeStruct((count, width), BF16),
            jax.ShapeDtypeStruct((experts, deep, LANES), dtype),
        ),
        (pltpu.VMEM((experts * deep, LANES), F32), pltpu.VMEM((count, width), F32)),
        mib=62,
        cost=12 * count * width * hidden,
        grid=(steps,),
        in_specs=[
            pl.BlockSpec((experts, deep, LANES), lambda j: (0, part, 0)),
            across, across, down, across, across, down,
        ],
        out_specs=(
            pl.BlockSpec((count, width), lambda j: (0, 0)),
            pl.BlockSpec((experts, deep, LANES), lambda j: (0, 0, 0)),
        ),
    )(flat, *mine, *other)


def factors_body(rows, gate, up, turned_rows, turned_hidden, by_gate, by_up):
    x = rows[...]
    pre_gate = jnp.dot(x, gate[0], preferred_element_type=F32)
    pre_up = jnp.dot(x, up[0], preferred_element_type=F32)
    s = jax.nn.sigmoid(pre_gate)
    through = pre_gate * s
    by_gate[...] = pre_up * s * (1.0 + pre_gate * (1.0 - s))
    by_up[...] = through
    turned_hidden[...] = (through * pre_up).astype(BF16).T
    turned_rows[...] = x.T


def factors(rows, gate, up):
    count, width = rows.shape
    hidden = gate.shape[2]
    cut = 256
    held = pl.BlockSpec((1, width, hidden), lambda i: (0, 0, 0))
    return call(
        factors_body,
        (
            jax.ShapeDtypeStruct((width, count), BF16),
            jax.ShapeDtypeStruct((hidden, count), BF16),
            jax.ShapeDtypeStruct((count, hidden), F32),
            jax.ShapeDtypeStruct((count, hidden), F32),
        ),
        mib=62,
        cost=4 * count * width * hidden,
        grid=(count // cut,),
        in_specs=[pl.BlockSpec((cut, width), lambda i: (i, 0)), held, held],
        out_specs=(
            pl.BlockSpec((width, cut), lambda i: (0, i)),
            pl.BlockSpec((hidden, cut), lambda i: (0, i)),
            pl.BlockSpec((cut, hidden), lambda i: (i, 0)),
            pl.BlockSpec((cut, hidden), lambda i: (i, 0)),
        ),
    )(rows, gate, up)


def mix_in(flat, latent, mixed, where, scratch, gathered):
    pieces = latent.shape[1] // LANES
    scratch[...] = flat[...].astype(F32).reshape(scratch.shape)
    for c in range(pieces):
        gathered[:, c * LANES : (c + 1) * LANES] = load_flat(scratch, pieces, c).astype(BF16)
    picked = [
        jnp.dot(where[k], gathered[...], preferred_element_type=F32) * mixed[k] for k in range(2)
    ]
    return latent[...].astype(F32) + (picked[0] + picked[1])


def student_body(
    experts, capacity, flat, latent, s_routes, t_routes, mixing, output, s_where, t_where, scratch,
    gathered,
):
    for routes, out in ((s_routes, s_where), (t_routes, t_where)):
        first, second = places(routes[...], experts, capacity)
        out[0] = first
        out[1] = second
    mixed = [column(mixing[...], k) for k in range(2)]
    output[...] = mix_in(flat, latent, mixed, s_where, scratch, gathered)


def combine_body(
    factor, flat, latent, student_out, s_where, t_where, s_mixing, t_mixing, packed, scratch,
    gathered,
):
    s_mixed, t_mixed = ([column(m[...], k) for k in range(2)] for m in (s_mixing, t_mixing))
    target_out = mix_in(flat, latent, t_mixed, t_where, scratch, gathered)
    cotangent = factor * (student_out[...] - target_out)
    slots = [turned_dot(s_where[k], (s_mixed[k] * cotangent).astype(BF16)) for k in range(2)]
    store_flat(slots[0] + slots[1], scratch)
    packed[...] = scratch[...].reshape(packed.shape).astype(BF16)


def backward_body(last, *refs):
    one, two, down, turned_rows, turned_hidden, by_gate, by_up = refs[:7]
    earlier = refs[7:10] if last else (None,) * 3
    gate_out, up_out, down_out, scratch, cotangent = refs[-5:]
    pieces = down.shape[2] // LANES

    @pl.when(pl.program_id(0) == 0)
    def _():
        count = cotangent.shape[0] // 2
        for b, flat in enumerate((one, two)):
            scratch[...] = flat[...].astype(F32).reshape(scratch.shape)
            for c in range(pieces):
                cotangent[b * count : (b + 1) * count, c * LANES : (c + 1) * LANES] = load_flat(
                    scratch, pieces, c
                ).astype(BF16)

    back = cotangent[...]
    grad_hidden = lax.dot_general(
        back, down[0], (((1,), (1,)), ((), ())), preferred_element_type=F32
    )
    grad_gate = (grad_hidden * by_gate[...]).astype(BF16)
    grad_up = (grad_hidden * by_up[...]).astype(BF16)
    for out, before, left, right in (
        (gate_out, earlier[0], turned_rows, grad_gate),
        (up_out, earlier[1], turned_rows, grad_up),
        (down_out, earlier[2], turned_hidden, back),
    ):
        found = jnp.dot(left[...], right, preferred_element_type=F32)
        out[0] = (found if before is None else found + before[0]).astype(out.dtype)


def backward(blocks, turn, down, turned_rows, turned_hidden, by_gate, by_up, earlier=()):
    steps = 2
    hidden, width = down.shape[1:]
    count = turned_rows.shape[1] // 2
    cut = hidden // steps
    dtype = BF16 if earlier else F32
    flat = pl.BlockSpec(blocks[0].shape, lambda j: (0, 0, 0))
    flat_rows = blocks[0].shape[0] * blocks[0].shape[1]
    grads = [
        pl.BlockSpec((1, width, cut), lambda j: (0, 0, j)),
        pl.BlockSpec((1, width, cut), lambda j: (0, 0, j)),
        pl.BlockSpec((1, cut, width), lambda j: (0, j, 0)),
    ]
    return call(
        functools.partial(backward_body, bool(earlier)),
        (
            jax.ShapeDtypeStruct((1, width, hidden), dtype),
            jax.ShapeDtypeStruct((1, width, hidden), dtype),
            jax.ShapeDtypeStruct((1, hidden, width), dtype),
        ),
        (pltpu.VMEM((flat_rows, LANES), F32), pltpu.VMEM((count, width), BF16)),
        cost=4 * count * 2 * width * hidden,
        grid=(steps,),
        in_specs=[
            flat, flat,
            pl.BlockSpec((1, cut, width), lambda j: (0, j, 0)),
            pl.BlockSpec((width, count), lambda j: (0, turn)),
            pl.BlockSpec((cut, count), lambda j: (j, turn)),
            pl.BlockSpec((count, cut), lambda j: (turn, j)),
            pl.BlockSpec((count, cut), lambda j: (turn, j)),
            *(grads if earlier else ()),
        ],
        out_specs=tuple(grads),
    )(*blocks, down, turned_rows, turned_hidden, by_gate, by_up, *earlier)


def to_experts(blocks):
    return lax.all_to_all(blocks, "expert", split_axis=0, concat_axis=0, tiled=True)


def other_core(value):
    return lax.ppermute(value, "dp", ((0, 1), (1, 0), (2, 3), (3, 2)))


def other_chip(value):
    return lax.ppermute(value, "dp", ((0, 2), (2, 0), (1, 3), (3, 1)))


def shards(
    student_latent,
    target_latent,
    student_gate,
    student_up,
    student_down,
    target_gate,
    target_up,
    target_down,
    student_routes,
    target_routes,
    student_mixing,
    target_mixing,
):
    groups = lax.axis_size("dp")
    experts = lax.axis_size("expert")
    tokens, width = student_latent.shape
    top = student_routes.shape[1]
    capacity = tokens * top * 5 // (4 * experts)
    slots = experts * capacity
    deep = capacity * width // LANES
    flat_shape = (experts * deep, LANES)
    blocks_shape = (experts, deep, LANES)

    def packing(*sets):
        return call(
            functools.partial(pack_body, experts, capacity),
            jax.ShapeDtypeStruct((experts, len(sets) // 2 * deep, LANES), BF16),
            (pltpu.VMEM(flat_shape, F32),),
            mib=12,
            cost=2 * tokens * slots * width,
        )(*sets)

    student_routes, target_routes = student_routes.T, target_routes.T
    student_mixing, target_mixing = student_mixing.T, target_mixing.T
    far_latent = other_chip(target_latent)
    far_routes = other_chip(target_routes)
    sent_student = packing(student_latent, student_routes)
    sent_target = packing(target_latent, target_routes, far_latent, far_routes)
    own_student = to_experts(sent_student)
    both_target = to_experts(sent_target)
    student = (student_gate, student_up, student_down)
    target = (target_gate, target_up, target_down)
    student2 = tuple(other_core(w) for w in student)
    target2 = tuple(other_core(w) for w in target)
    far_student = other_chip(own_student)

    own_rows, own_part = forward(own_student, 0, 1, student, student2, width, F32)
    far_rows, far_part = forward(far_student, 0, 1, student, student2, width, BF16)
    own_part_t = forward(both_target, 0, 2, target, target2, width, F32)[1]
    far_part_t = forward(both_target, 1, 2, target, target2, width, BF16)[1]
    came_s = other_chip(far_part)
    came_t = other_chip(far_part_t)
    student_sum = (own_part + came_s.astype(F32)).astype(BF16)
    target_sum = (own_part_t + came_t.astype(F32)).astype(BF16)
    back_student = to_experts(student_sum)
    back_target = to_experts(target_sum)

    rows = jnp.concatenate([own_rows, other_core(own_rows), far_rows, other_core(far_rows)], axis=0)
    turned_rows, turned_hidden, by_gate, by_up = factors(rows, student_gate, student_up)

    factor = (experts / (top * tokens * groups * experts)) ** 0.5
    room = (pltpu.VMEM(flat_shape, F32), pltpu.VMEM((slots, width), BF16))
    where = jax.ShapeDtypeStruct((top, tokens, slots), BF16)
    student_out, s_where, t_where = call(
        functools.partial(student_body, experts, capacity),
        (jax.ShapeDtypeStruct((tokens, width), F32), where, where),
        room,
        mib=62,
        cost=4 * tokens * slots * width,
    )(back_student, student_latent, student_routes, target_routes, student_mixing)
    slot_values = call(
        functools.partial(combine_body, factor),
        jax.ShapeDtypeStruct(blocks_shape, BF16),
        room,
        mib=62,
        cost=8 * tokens * slots * width,
    )(
        back_target, target_latent, student_out, s_where, t_where, student_mixing,
        target_mixing,
    )
    own_cot = to_experts(slot_values)
    far_cot = other_chip(own_cot)
    own_cot2 = other_core(own_cot)
    given = (student_down, turned_rows, turned_hidden, by_gate, by_up)
    near = backward((own_cot, own_cot2), 0, *given)
    far_cot2 = other_core(far_cot)
    return backward((far_cot, far_cot2), 1, *given, tuple(near))


def solution(mesh):
    in_specs = (
        P(("dp", "expert"), None),
        P(("dp", "expert"), None),
        P("expert", None, "dp"),
        P("expert", None, "dp"),
        P("expert", "dp", None),
        P("expert", None, "dp"),
        P("expert", None, "dp"),
        P("expert", "dp", None),
        P(("dp", "expert"), None),
        P(("dp", "expert"), None),
        P(("dp", "expert"), None),
        P(("dp", "expert"), None),
    )
    out_specs = (P("expert", None, "dp"), P("expert", None, "dp"), P("expert", "dp", None))
    return jax.shard_map(shards, mesh=mesh, in_specs=in_specs, out_specs=out_specs, check_vma=False)
```
